32 devices in a mesh: tm: 16 (over z, y, core), space: 2 (over x).
Axes of the slice: x: 2, y: 2, z: 4, core: 2. Of those that a mesh axis runs over, the one named last changes fastest.
Arguments:
- forcing: float32 [32, 128, 128, 128], P('tm', 'space'), may hold values from -24 to 24
- exponents: int32 [32], P('tm'), may hold values from 0 to 8
- mixing: float32 [32, 32], replicated, may hold values from -1 to 3, as said below
- unmixing: float32 [32, 32], replicated, may hold values from -1 to 1
Outputs:
- solution: float32 [32, 128, 128, 128], P('tm', 'space')
The draws below stay inside these ranges and needn't reach their ends.
Inputs may be any that keep to these rules, and one draw needn't show every extreme that they name: unmixing is the inverse of mixing up to float32 rounding.
All inputs are finite; a program needn't handle non-finite values.
Results may differ from the reference program's by a relative error of at most 0.00027.
Values sent between devices are 32-bit elements; how exact they have to be, the bound alone decides.
A program may use at most 128 MiB of HBM per device.

```python
import math
import jax
import jax.numpy as jnp
from jax import lax

N = 128
STEPS = 32


def shared_pair(key):
    order = STEPS
    folded = jax.random.fold_in(key, 4711)
    diagonal_key, offdiag_key = jax.random.split(folded)
    diagonal = jax.random.uniform(diagonal_key, (order,), jnp.float32, 1.2, 2.0)
    offdiag = jnp.clip(jax.random.normal(offdiag_key, (order, order), jnp.float32), -4.0, 4.0)
    matrix = jnp.diag(diagonal) + 0.4 / math.sqrt(order) * offdiag
    inverse = jnp.linalg.solve(matrix, jnp.eye(order, dtype=jnp.float32))
    return (matrix, inverse)


def draw_mixing(key, part):
    return shared_pair(key)[0]


def draw_unmixing(key, part):
    return shared_pair(key)[1]


def draw_forcing(key, part):
    folded = jax.random.fold_in(key, 913)
    rough_key, amp_key = jax.random.split(folded)
    return jnp.clip(4.0 * jax.random.normal(rough_key, (STEPS, N, N, N), jnp.float32), -24.0, 24.0)


def plant(entries, rng, least, largest):
    extent = entries.shape
    place = [jax.random.randint(jax.random.fold_in(rng, axis), (), 0, extent[axis]) for axis in range(len(extent))]
    entries = entries.at[tuple(place)].set(least)
    longest = extent.index(max(extent))
    place[longest] = (place[longest] + 1) % extent[longest]
    return entries.at[tuple(place)].set(largest)


def setup_inputs(seed: int = 0) -> dict:
    streams_of = jax.random.split(jax.random.key(seed), 5)
    forcing = draw_forcing(jax.random.fold_in(streams_of[4], 71), 0)
    exponents = plant(jax.random.randint(streams_of[1], (STEPS,), 0, 9), jax.random.fold_in(streams_of[1], 1), 0, 8).astype(jnp.int32)
    mixing = draw_mixing(jax.random.fold_in(streams_of[4], 71), 0)
    unmixing = draw_unmixing(jax.random.fold_in(streams_of[4], 71), 0)
    return dict(forcing=forcing, exponents=exponents, mixing=mixing, unmixing=unmixing)


exact_mode = lax.Precision.HIGHEST

def sine_matrix(length):
    ordinal = jnp.arange(length, dtype=jnp.float32) + 1.0
    angle_step = jnp.pi / (length + 1)
    return jnp.sqrt(2.0 / (length + 1.0)) * jnp.sin(angle_step * ordinal[:, None] * ordinal[None, :])

def eigen_values(length):
    ordinal = jnp.arange(length, dtype=jnp.float32) + 1.0
    return 2.0 - 2.0 * jnp.cos(jnp.pi * ordinal / (length + 1))

def transform(grid_field, matrix):
    grid_field = jnp.einsum('abc,ak->kbc', grid_field, matrix, precision=exact_mode)
    grid_field = jnp.einsum('abc,bk->akc', grid_field, matrix, precision=exact_mode)
    return jnp.dot(grid_field, matrix, precision=exact_mode)

def reference(forcing, exponents, mixing, unmixing):
    step_count = forcing.shape[0]
    length = forcing.shape[1]
    transform_matrix = sine_matrix(length)
    eigen_all = eigen_values(length)
    denom_base = eigen_all[:, None, None] + eigen_all[None, :, None] + eigen_all[None, None, :]
    shifts = 2.0 ** (exponents.astype(jnp.float32) / 4.0)
    unmixed = jnp.dot(unmixing, forcing.reshape(step_count, -1), precision=exact_mode).reshape(forcing.shape)

    def solve_one(packed):
        grid_field, shift_val = packed
        spectral_field = transform(grid_field, transform_matrix)
        return transform(spectral_field / (shift_val + denom_base), transform_matrix)
    solved_field = lax.map(solve_one, (unmixed, shifts))
    return jnp.dot(mixing, solved_field.reshape(step_count, -1), precision=exact_mode).reshape(forcing.shape)
```

```python
import jax
import jax.numpy as jnp
from jax import lax
from jax.sharding import PartitionSpec as P

split_mode = lax.Precision.HIGH


def sine_matrix(length):
    ordinal = jnp.arange(length, dtype=jnp.float32) + 1.0
    angle_step = jnp.pi / (length + 1)
    return jnp.sqrt(2.0 / (length + 1.0)) * jnp.sin(
        angle_step * ordinal[:, None] * ordinal[None, :]
    )


def eigen_values(length):
    ordinal = jnp.arange(length, dtype=jnp.float32) + 1.0
    return 2.0 - 2.0 * jnp.cos(jnp.pi * ordinal / (length + 1))


def product(formula, left, right):
    return jnp.einsum(formula, left, right, precision=split_mode)


def body(times, slabs, forcing, exponents, mixing, unmixing):
    own_steps, slab, length, _ = forcing.shape
    devices = times * slabs
    rows = max(1, length // devices)
    pieces = max(1, devices // length)
    width = length // pieces
    everyone = ("tm", "space")
    sine = sine_matrix(length)
    eigen = eigen_values(length)
    all_exponents = lax.all_gather(exponents, "tm", axis=0, tiled=True)
    shifts = 2.0 ** (all_exponents.astype(jnp.float32) / 4.0)

    field = product("labc,ck->labk", forcing, sine)
    field = product("labk,bj->jlak", field, sine)
    field = field.reshape(length, own_steps, slab, pieces, width).transpose(0, 3, 1, 2, 4)
    field = field.reshape(length * pieces, own_steps, slab, width)
    field = lax.all_to_all(field, everyone, split_axis=0, concat_axis=0, tiled=True)
    field = field.reshape(times, slabs, rows, own_steps, slab, width)
    field = field.transpose(2, 0, 3, 1, 4, 5).reshape(rows, times * own_steps, length, width)

    field = product("lm,jmak->jlak", unmixing, field)
    field = product("jlak,ai->jlik", field, sine)
    device = lax.axis_index("tm") * slabs + lax.axis_index("space")
    own_rows = lax.dynamic_slice_in_dim(eigen, device * rows // pieces, rows)
    own_columns = lax.dynamic_slice_in_dim(eigen, device % pieces * width, width)
    denom = (
        shifts[None, :, None, None]
        + eigen[None, None, :, None]
        + own_rows[:, None, None, None]
        + own_columns[None, None, None, :]
    )
    field = product("jlik,ia->jlak", field / denom, sine)
    field = product("lm,jmak->jlak", mixing, field)

    field = field.reshape(rows, times, own_steps, slabs, slab, width)
    field = field.transpose(1, 3, 0, 2, 4, 5).reshape(length * pieces, own_steps, slab, width)
    field = lax.all_to_all(field, everyone, split_axis=0, concat_axis=0, tiled=True)
    field = field.reshape(length, pieces, own_steps, slab, width).transpose(0, 2, 3, 1, 4)
    field = field.reshape(length, own_steps, slab, length)
    field = product("jlak,jb->labk", field, sine)
    return product("labk,kc->labc", field, sine)


def solution(mesh):
    placed = (P("tm", "space", None, None), P("tm"), P(), P())

    def run(*arrays):
        return body(mesh.shape["tm"], mesh.shape["space"], *arrays)

    return jax.shard_map(
        run, mesh=mesh, in_specs=placed, out_specs=P("tm", "space", None, None), check_vma=False
    )
```

```python
import jax
import jax.numpy as jnp
from jax import lax
from jax.sharding import PartitionSpec as P

split_mode = lax.Precision.HIGH


def sine_matrix(length):
    ordinal = jnp.arange(length, dtype=jnp.float32) + 1.0
    angle_step = jnp.pi / (length + 1)
    return jnp.sqrt(2.0 / (length + 1.0)) * jnp.sin(
        angle_step * ordinal[:, None] * ordinal[None, :]
    )


def eigen_values(length):
    ordinal = jnp.arange(length, dtype=jnp.float32) + 1.0
    return 2.0 - 2.0 * jnp.cos(jnp.pi * ordinal / (length + 1))


def product(formula, left, right):
    return jnp.einsum(formula, left, right, precision=split_mode)


def body(times, slabs, chunks, forcing, exponents, mixing, unmixing):
    own_steps, slab, length, _ = forcing.shape
    devices = times * slabs
    part = length // chunks
    rows = max(1, part // devices)
    pieces = max(1, devices // part)
    width = length // pieces
    everyone = ("tm", "space")
    sine = sine_matrix(length)
    eigen = eigen_values(length)
    all_exponents = lax.all_gather(exponents, "tm", axis=0, tiled=True)
    first_sine, all_exponents = lax.optimization_barrier((sine, all_exponents))
    shifts = 2.0 ** (all_exponents.astype(jnp.float32) / 4.0)
    device = lax.axis_index("tm") * slabs + lax.axis_index("space")
    own_columns = lax.dynamic_slice_in_dim(eigen, device % pieces * width, width)

    def spread(field, chunk):
        own_sine = first_sine[:, chunk * part : (chunk + 1) * part]
        field = product("labk,bj->jlak", field, own_sine)
        field = field.reshape(part, own_steps, slab, pieces, width).transpose(0, 3, 1, 2, 4)
        field = field.reshape(part * pieces, own_steps, slab, width)
        return lax.all_to_all(field, everyone, split_axis=0, concat_axis=0, tiled=True)

    def solve(field, chunk):
        field = field.reshape(times, slabs, rows, own_steps, slab, width)
        field = field.transpose(2, 0, 3, 1, 4, 5).reshape(rows, times * own_steps, length, width)
        field = product("lm,jmak->jlak", unmixing, field)
        field = product("jlak,ai->jlik", field, sine)
        first = chunk * part + device * rows // pieces
        own_rows = lax.dynamic_slice_in_dim(eigen, first, rows)
        denom = (
            shifts[None, :, None, None]
            + eigen[None, None, :, None]
            + own_rows[:, None, None, None]
            + own_columns[None, None, None, :]
        )
        field = product("jlik,ia->jlak", field / denom, sine)
        field = product("lm,jmak->jlak", mixing, field)
        field = field.reshape(rows, times, own_steps, slabs, slab, width)
        field = field.transpose(1, 3, 0, 2, 4, 5).reshape(part * pieces, own_steps, slab, width)
        return lax.all_to_all(field, everyone, split_axis=0, concat_axis=0, tiled=True)

    def gather(field, chunk):
        field = field.reshape(part, pieces, own_steps, slab, width).transpose(0, 2, 3, 1, 4)
        field = field.reshape(part, own_steps, slab, length)
        return product("jlak,jb->labk", field, sine[chunk * part : (chunk + 1) * part])

    field = product("labc,ck->labk", forcing, sine)
    sent = [spread(field, chunk) for chunk in range(chunks)]
    solved = [solve(held, chunk) for chunk, held in enumerate(sent)]
    field = sum(gather(held, chunk) for chunk, held in enumerate(solved))
    return product("labk,kc->labc", field, sine)


def solution(mesh):
    placed = (P("tm", "space", None, None), P("tm"), P(), P())

    def run(*arrays):
        return body(mesh.shape["tm"], mesh.shape["space"], 2, *arrays)

    return jax.shard_map(
        run, mesh=mesh, in_specs=placed, out_specs=P("tm", "space", None, None), check_vma=False
    )
```
